128 devices in a mesh: dp: 1, col: 16 (over z, y), row: 8 (over x, core).
Axes of the slice: x: 4, y: 4, z: 4, core: 2. Of those that a mesh axis runs over, the one named last changes fastest.
Arguments:
- x_in: bfloat16 [4096, 4096], P(('dp', 'row'), 'col')
- w_qkv: bfloat16 [4096, 12288], P('row', 'col')
- w_out: bfloat16 [4096, 4096], P('row', 'col')
- doc_ids: int32 [4096], P(('dp', 'row'))
- grad_y: bfloat16 [4096, 4096], P(('dp', 'row'), 'col')
Outputs:
- output 1: bfloat16 [4096, 4096], P(('dp', 'row'), 'col')
- output 2: bfloat16 [4096, 12288], P(('dp', 'row'), 'col')
- output 3: bfloat16 [4096, 4096], P(('dp', 'row'), 'col')
All inputs are finite; a program needn't handle non-finite values.
Results may differ from the reference program's by a relative error of at most 0.00407559.
Values are sent between devices in bfloat16 or wider.
A program may use at most 1 GiB of HBM per device.

```python
import jax
import jax.numpy as jnp
from jax import lax

TOKENS = 4096
HIDDEN = 4096
HEADS = 32
HEAD_DIM = 128
QUERY_BLOCK = 256
DOCS = 3


def setup_inputs(seed: int = 0, part: int = 0) -> dict:
    part_key = jax.random.fold_in(jax.random.key(seed), part)
    key_x, key_doc, key_dy = jax.random.split(part_key, 3)
    key_wq, key_wo = jax.random.split(jax.random.key(seed + 1), 2)
    x_in = jax.random.normal(key_x, (TOKENS, HIDDEN), jnp.float32).astype(jnp.bfloat16)
    w_qkv = (jax.random.normal(key_wq, (HIDDEN, 3 * HIDDEN), jnp.float32) * HIDDEN ** -0.5).astype(jnp.bfloat16)
    w_out = (jax.random.normal(key_wo, (HIDDEN, HIDDEN), jnp.float32) * HIDDEN ** -0.5).astype(jnp.bfloat16)
    doc_cuts = jax.random.randint(key_doc, (DOCS - 1,), 1, TOKENS)
    doc_ids = jnp.sum(jnp.arange(TOKENS)[:, None] >= doc_cuts[None, :], axis=1).astype(jnp.int32)
    grad_y = jax.random.normal(key_dy, (TOKENS, HIDDEN), jnp.float32).astype(jnp.bfloat16)
    return {'x_in': x_in, 'w_qkv': w_qkv, 'w_out': w_out, 'doc_ids': doc_ids, 'grad_y': grad_y}


def reference(x_in, w_qkv, w_out, doc_ids, grad_y):
    sm_scale = HEAD_DIM ** -0.5
    n_blocks = TOKENS // QUERY_BLOCK
    qkv_all = jnp.dot(x_in, w_qkv, preferred_element_type=jnp.float32).astype(jnp.bfloat16)
    qkv_heads = jnp.transpose(qkv_all.reshape(TOKENS, HEADS, 3, HEAD_DIM), (1, 2, 0, 3))
    d_attn = jnp.dot(grad_y, w_out.T, preferred_element_type=jnp.float32).astype(jnp.bfloat16)
    dattn_heads = jnp.transpose(d_attn.reshape(TOKENS, HEADS, HEAD_DIM), (1, 0, 2))
    seg_blocks = doc_ids.reshape(n_blocks, QUERY_BLOCK)

    def one_head(head_args):
        qkv_head, do_head = head_args
        q_head = qkv_head[0]
        k_head = qkv_head[1]
        v_head = qkv_head[2]

        def one_block(acc_pair, blk_args):
            dk_acc, dv_acc = acc_pair
            q_blk, do_blk, seg_blk = blk_args
            scores = jnp.dot(q_blk, k_head.T, preferred_element_type=jnp.float32) * sm_scale
            scores = jnp.where(seg_blk[:, None] == doc_ids[None, :], scores, -jnp.inf)
            p_attn = jax.nn.softmax(scores, axis=-1)
            p_bf = p_attn.astype(jnp.bfloat16)
            o_blk = jnp.dot(p_bf, v_head, preferred_element_type=jnp.float32).astype(jnp.bfloat16)
            d_probs = jnp.dot(do_blk, v_head.T, preferred_element_type=jnp.float32)
            row_dot = jnp.sum(p_attn * d_probs, axis=-1, keepdims=True)
            d_scores = (p_attn * (d_probs - row_dot) * sm_scale).astype(jnp.bfloat16)
            dq_blk = jnp.dot(d_scores, k_head, preferred_element_type=jnp.float32)
            dk_acc = dk_acc + jnp.dot(d_scores.T, q_blk, preferred_element_type=jnp.float32)
            dv_acc = dv_acc + jnp.dot(p_bf.T, do_blk, preferred_element_type=jnp.float32)
            return (dk_acc, dv_acc), (o_blk, dq_blk)

        zero_acc = jnp.zeros((TOKENS, HEAD_DIM), jnp.float32)
        blk_inputs = (q_head.reshape(n_blocks, QUERY_BLOCK, HEAD_DIM), do_head.reshape(n_blocks, QUERY_BLOCK, HEAD_DIM), seg_blocks)
        (dk_head, dv_head), (o_head, dq_head) = lax.scan(one_block, (zero_acc, zero_acc), blk_inputs)
        dqkv_head = jnp.stack([dq_head.reshape(TOKENS, HEAD_DIM), dk_head, dv_head])
        return o_head.reshape(TOKENS, HEAD_DIM), dqkv_head

    attn_heads, dqkv_heads = lax.map(one_head, (qkv_heads, dattn_heads))
    attn_out = jnp.transpose(attn_heads, (1, 0, 2)).reshape(TOKENS, HIDDEN)
    d_qkv = jnp.transpose(dqkv_heads, (2, 0, 1, 3)).reshape(TOKENS, 3 * HIDDEN).astype(jnp.bfloat16)
    grad_x = jnp.dot(d_qkv, w_qkv.T, preferred_element_type=jnp.float32).astype(jnp.bfloat16)
    grad_wqkv = jnp.dot(x_in.T, d_qkv, preferred_element_type=jnp.float32).astype(jnp.bfloat16)
    grad_wout = jnp.dot(attn_out.T, grad_y, preferred_element_type=jnp.float32).astype(jnp.bfloat16)
    return (grad_x, grad_wqkv, grad_wout)
```

```python
import jax
import jax.numpy as jnp
from jax import lax
from jax.experimental import pallas as pl
from jax.experimental.pallas import tpu as pltpu
from jax.sharding import PartitionSpec as P

HEAD_DIM = 128
NR, NC = 8, 16
SB = 512
SCALE = HEAD_DIM ** -0.5
HB, LANE, QKV, HQKV = 256, 128, 768, 384
MESH = pl.DeviceIdType.MESH
BF = jnp.bfloat16
F32 = jnp.float32
NT = (((1,), (1,)), ((), ()))
TN = (((0,), (0,)), ((), ()))
VLIM = 60 * 1024 * 1024


def dot(a, b, dims=None):
    if dims is None:
        dims = (((1,), (0,)), ((), ()))
    return lax.dot_general(a, b, dims, preferred_element_type=F32)


class Net:
    def __init__(self, send, recv):
        self.send, self.recv, self.n = send, recv, 0
        self.c, self.r = lax.axis_index('col'), lax.axis_index('row')
        self.x, self.core = self.r // 2, self.r % 2
        self.z, self.y = self.c // 4, self.c % 4
        self.sent = []

    def dev(self, axis, step):
        x, z, y, core = self.x, self.z, self.y, self.core
        if axis == 'x':
            x = (x + step) % 4
        elif axis == 'z':
            z = (z + step) % 4
        elif axis == 'y':
            y = (y + step) % 4
        else:
            core = 1 - core
        return {'col': z * 4 + y, 'row': x * 2 + core}

    def copy(self, src, dst, dev):
        i = self.n
        self.n += 1
        cp = pltpu.make_async_remote_copy(
            src_ref=src, dst_ref=dst, send_sem=self.send.at[i], recv_sem=self.recv.at[i],
            device_id=dev, device_id_type=MESH)
        cp.start()
        self.sent.append(cp)
        return cp

    def enter(self, axes, swap):
        bar = pltpu.get_barrier_semaphore()
        peers = []
        for a in axes:
            peers += [self.dev(a, 1), self.dev(a, 3)] if a != 'core' else [self.dev(a, 1)]
        for d in peers:
            pl.semaphore_signal(bar, inc=1, device_id=d, device_id_type=MESH)
        if swap:
            for k in range(2):
                @pl.when(jnp.logical_not(self.own_swap(k)))
                def _():
                    pl.semaphore_signal(bar, inc=1, device_id=self.swap_dev(k), device_id_type=MESH)
            n = len(peers) + 2 - (self.c // 2 == self.r).astype(jnp.int32)
            pl.semaphore_wait(bar, n)
        else:
            pl.semaphore_wait(bar, len(peers))

    def own_swap(self, k):
        return jnp.logical_and(self.c // 2 == self.r, self.c % 2 == k)

    def swap_dev(self, k):
        return {'col': 2 * self.r + k, 'row': self.c // 2}

    def finish(self):
        for cp in self.sent:
            cp.wait_send()


def swap_steps(net, src, dst, base):
    i = net.c % 2

    def cp(k, slot):
        return pltpu.make_async_remote_copy(
            src_ref=src.at[k], dst_ref=dst.at[slot], send_sem=net.send.at[base + k],
            recv_sem=net.recv.at[base + slot], device_id=net.swap_dev(k), device_id_type=MESH)

    for k in range(2):
        own = net.own_swap(k)

        @pl.when(jnp.logical_not(own))
        def _():
            cp(k, i).start()

        @pl.when(own)
        def _():
            dst[k] = src[k]
    yield
    for k in range(2):
        @pl.when(jnp.logical_not(net.own_swap(k)))
        def _():
            cp(k, k).wait_recv()
    net.tail.append(lambda: [pl.when(jnp.logical_not(net.own_swap(k)))(lambda k=k: cp(k, k).wait_send()) for k in range(2)])


def row_steps(net, src, out, half, local):
    x, core = net.x, net.core
    slot = lambda s: out.at[((x + s) % 4) * 2 + core]
    me = out.at[net.r]
    right, left, mate = net.dev('x', 1), net.dev('x', 3), net.dev('core', 1)
    a = net.copy(src, me, right)
    b = net.copy(src, me, left)
    got = [net.copy(src, me, mate)]
    own = pltpu.make_async_copy(src, me, local)
    own.start()
    yield
    a.wait_recv()
    c = net.copy(half(slot(3), 0), half(slot(3), 0), right)
    got.append(net.copy(slot(3), slot(3), mate))
    b.wait_recv()
    d = net.copy(half(slot(1), 1), half(slot(1), 1), left)
    got.append(net.copy(slot(1), slot(1), mate))
    yield
    c.wait_recv()
    d.wait_recv()
    got.append(net.copy(slot(2), slot(2), mate))
    yield
    for g in got:
        g.wait_recv()
    own.wait()


def col_steps(net, src, out, h, local):
    first, second = ('y', 'z') if h == 0 else ('z', 'y')
    z, y = net.z, net.y

    def one(s):
        return out.at[z, (y + s) % 4, h] if h == 0 else out.at[(z + s) % 4, y, h]

    def four(s):
        return out.at[(z + s) % 4, pl.ds(0, 4), h] if h == 0 else out.at[pl.ds(0, 4), (y + s) % 4, h]

    def pair(s, k):
        return out.at[(z + s) % 4, pl.ds(2 * k, 2), h] if h == 0 else out.at[pl.ds(2 * k, 2), (y + s) % 4, h]

    def rows(ref, k):
        return ref.at[pl.ds(k * LANE, LANE)]

    right, left = net.dev(first, 1), net.dev(first, 3)
    a = net.copy(src.at[h], one(0), right)
    b = net.copy(src.at[h], one(0), left)
    own = pltpu.make_async_copy(src.at[h], one(0), local)
    own.start()
    yield
    a.wait_recv()
    c = net.copy(rows(one(3), 0), rows(one(3), 0), right)
    b.wait_recv()
    d = net.copy(rows(one(1), 1), rows(one(1), 1), left)
    yield
    own.wait()
    c.wait_recv()
    d.wait_recv()
    right, left = net.dev(second, 1), net.dev(second, 3)
    a = net.copy(four(0), four(0), right)
    b = net.copy(four(0), four(0), left)
    yield
    a.wait_recv()
    c = net.copy(pair(3, 0), pair(3, 0), right)
    b.wait_recv()
    d = net.copy(pair(1, 1), pair(1, 1), left)
    yield
    c.wait_recv()
    d.wait_recv()


def drive(net, *groups):
    live = list(groups)
    while live:
        nxt = []
        for g in live:
            try:
                next(g)
                nxt.append(g)
            except StopIteration:
                pass
        live = nxt
    net.finish()
    for f in net.tail:
        f()


def later(steps, n):
    next(steps)
    yield
    for _ in range(n):
        yield
    yield from steps


def half_rows(n):
    return lambda ref, h: ref.at[pl.ds(h * n, n)]


def half_lead(ref, h):
    return ref.at[h]


def gather_in(x, dy, w, wo, seg, xg, dyg, wg, wog, segg, xt, dyt, wot, send, recv, local):
    net = Net(send, recv)
    net.tail = []
    net.enter(('x', 'z', 'y', 'core'), True)
    net.n = 6

    def wo_all():
        yield from swap_steps(net, wo, wot, 0)
        yield from later(row_steps(net, wot, wog, half_lead, local.at[0]), 1)

    drive(net,
          wo_all(),
          col_steps(net, x, xg, 0, local.at[1]), col_steps(net, x, xg, 1, local.at[2]),
          col_steps(net, dy, dyg, 0, local.at[5]), col_steps(net, dy, dyg, 1, local.at[6]),
          later(row_steps(net, seg, segg, half_rows(4), local.at[4]), 1),
          later(row_steps(net, w, wg, half_rows(HB), local.at[3]), 1),
          later(swap_steps(net, x, xt, 2), 5), later(swap_steps(net, dy, dyt, 4), 5))


def gather_mid(qkvo, xt, dyt, ag, xtg, dytg, send, recv, local):
    net = Net(send, recv)
    net.tail = []
    net.enter(('x', 'z', 'y', 'core'), False)
    drive(net,
          col_steps(net, xt, xtg, 0, local.at[1]), col_steps(net, xt, xtg, 1, local.at[2]),
          col_steps(net, dyt, dytg, 0, local.at[3]), col_steps(net, dyt, dytg, 1, local.at[4]),
          later(row_steps(net, qkvo, ag, half_rows(HB), local.at[0]), 1))


def gather_out(o, st, og, sg, send, recv, local):
    net = Net(send, recv)
    net.tail = []
    net.enter(('x', 'core'), False)
    drive(net,
          row_steps(net, st, sg, lambda ref, h: ref.at[:, pl.ds(h * HB, HB)], local.at[0]),
          row_steps(net, o, og, half_rows(HB), local.at[1]))


def scatter_steps(net, h, dq, w, dx, s1, r1, s2, r2, own, r3, r4):
    first, second = ('z', 'y') if h == 0 else ('y', 'z')
    f, g = (net.z, net.y) if h == 0 else (net.y, net.z)

    def part(ft, gt):
        c = ft * 4 + gt if h == 0 else gt * 4 + ft
        wb = w[c // 2, pl.ds(pl.multiple_of((c % 2) * HB, HB), HB), :]
        return dot(dq[pl.ds(h * HB, HB), :], wb, NT)

    def fill(dst, ft, base):
        def body(j, _):
            dst[j] = part(ft, base + j)
            return 0
        lax.fori_loop(0, dst.shape[0], body, 0)

    right, left = net.dev(first, 1), net.dev(first, 3)
    fill(s1.at[0], (f + 2) % 4, 0)
    fill(s1.at[1], (f + 2) % 4, 2)
    a = net.copy(s1.at[0], r1.at[0], right)
    b = net.copy(s1.at[1], r1.at[1], left)
    yield
    fill(s2.at[0], (f + 1) % 4, 0)
    fill(s2.at[1], (f + 3) % 4, 0)
    yield
    a.wait_recv()

    def add0(j, _):
        s2[0, j] = s2[0, j] + r1[0, j]
        return 0
    lax.fori_loop(0, 2, add0, 0)
    b.wait_recv()

    def add1(j, _):
        s2[1, 2 + j] = s2[1, 2 + j] + r1[1, j]
        return 0
    lax.fori_loop(0, 2, add1, 0)
    a = net.copy(s2.at[0], r2.at[0], right)
    b = net.copy(s2.at[1], r2.at[1], left)
    fill(own, f, 0)
    yield
    a.wait_recv()
    b.wait_recv()

    def add2(j, _):
        own[j] = own[j] + r2[0, j] + r2[1, j]
        return 0
    lax.fori_loop(0, 4, add2, 0)
    right, left = net.dev(second, 1), net.dev(second, 3)
    go, gr, gl = (g + 2) % 4, (g + 1) % 4, (g + 3) % 4
    a = net.copy(own.at[go, pl.ds(0, LANE)], r3.at[0], right)
    b = net.copy(own.at[go, pl.ds(LANE, LANE)], r3.at[1], left)
    yield
    a.wait_recv()
    own[gr, pl.ds(0, LANE), :] = own[gr, pl.ds(0, LANE), :] + r3[0]
    b.wait_recv()
    own[gl, pl.ds(LANE, LANE), :] = own[gl, pl.ds(LANE, LANE), :] + r3[1]
    a = net.copy(own.at[gr], r4.at[0], right)
    b = net.copy(own.at[gl], r4.at[1], left)
    yield
    a.wait_recv()
    b.wait_recv()
    dx[h] = (own[g] + r4[0] + r4[1]).astype(BF)


def scatter_out(dq, w, dwo, dx, dqg, dwt, *scr):
    bufs, (send, recv, local) = scr[:14], scr[14:]
    net = Net(send, recv)
    net.tail = []
    net.enter(('x', 'z', 'y', 'core'), True)
    net.n = 2
    drive(net,
          later(row_steps(net, dq, dqg, half_rows(HB), local.at[0]), 2),
          scatter_steps(net, 0, dq, w, dx, *bufs[:7]), scatter_steps(net, 1, dq, w, dx, *bufs[7:]),
          later(swap_steps(net, dwo, dwt, 0), 3))


def project(x, w, dy, wo, out, acc, acc2):
    i = pl.program_id(0)

    @pl.when(i == 0)
    def _():
        acc[...] = jnp.zeros_like(acc)
        acc2[...] = jnp.zeros_like(acc2)

    acc[...] += dot(x[0].reshape(SB, HB), w[0, pl.ds(0, HB), :]) + dot(x[1].reshape(SB, HB), w[0, pl.ds(HB, HB), :])
    acc2[...] += dot(dy[0].reshape(SB, HB), wo[0, 0], NT) + dot(dy[1].reshape(SB, HB), wo[0, 1], NT)

    @pl.when(i == NR - 1)
    def _():
        out[:, pl.ds(0, QKV)] = acc[...].astype(BF)
        out[:, pl.ds(QKV, HB)] = acc2[...].astype(BF)


def doc_of(pos, c1, c2):
    return (pos >= c1).astype(jnp.int32) + (pos >= c2).astype(jnp.int32)


def bounds(r, c1, c2):
    p0, p1 = r * SB, r * SB + SB - 1
    lo = jnp.where(p0 >= c2, c2, jnp.where(p0 >= c1, c1, 0))
    hi = jnp.where(p1 >= c2, NR * SB, jnp.where(p1 >= c1, c2, c1))
    return lo // SB, (hi + SB - 1) // SB


def tile(t):
    return slice(t * LANE, (t + 1) * LANE)


def attend(cuts, ag, o, dq, st, s_scr, d_scr, m_scr, l_scr, e_scr, o_scr, q_scr):
    r = lax.axis_index('row')
    c1, c2 = cuts[0], cuts[1]
    lo, hi = bounds(r, c1, c2)
    qdoc = doc_of(r * SB + lax.broadcasted_iota(jnp.int32, (SB, LANE), 0), c1, c2)
    st[...] = jnp.zeros_like(st)
    for h in range(2):
        b = h * HQKV
        m_scr[...] = jnp.full(m_scr.shape, -jnp.inf, F32)
        l_scr[...] = jnp.zeros_like(l_scr)
        e_scr[...] = jnp.zeros_like(e_scr)
        o_scr[...] = jnp.zeros_like(o_scr)
        q_scr[...] = jnp.zeros_like(q_scr)

        def sweep1(kb, _):
            s = dot(ag[r, :, b:b + LANE], ag[kb, :, b + LANE:b + HB], NT) * SCALE
            m = m_scr[...]
            for t in range(4):
                kdoc = doc_of(kb * SB + t * LANE + lax.broadcasted_iota(jnp.int32, (1, LANE), 1), c1, c2)
                v = jnp.where(qdoc == kdoc, s[:, tile(t)], -jnp.inf)
                s_scr[kb, :, tile(t)] = v
                m = jnp.maximum(m, v)
            m_scr[...] = m
            return 0
        lax.fori_loop(lo, hi, sweep1, 0)
        m_scr[...] = jnp.broadcast_to(jnp.max(m_scr[...], axis=1, keepdims=True), m_scr.shape)

        def sweep2(kb, _):
            d = dot(ag[r, :, QKV + h * LANE:896 + h * LANE], ag[kb, :, b + HB:b + HQKV], NT)
            l, e, m = l_scr[...], e_scr[...], m_scr[...]
            for t in range(4):
                p = jnp.exp(s_scr[kb, :, tile(t)] - m)
                s_scr[kb, :, tile(t)] = p
                d_scr[kb, :, tile(t)] = d[:, tile(t)]
                l = l + p
                e = e + p * d[:, tile(t)]
            l_scr[...] = l
            e_scr[...] = e
            return 0
        lax.fori_loop(lo, hi, sweep2, 0)
        tot = jnp.sum(l_scr[...], axis=1, keepdims=True)
        dot_row = jnp.sum(e_scr[...], axis=1, keepdims=True) / tot
        lse = jnp.broadcast_to(m_scr[:, 0:1] + jnp.log(tot), m_scr.shape)
        st[h:h + 1, :] = jnp.transpose(lse)[0:1, :]
        l_scr[...] = jnp.broadcast_to(1.0 / tot, l_scr.shape)
        e_scr[...] = jnp.broadcast_to(dot_row, e_scr.shape)
        st[2 + h:3 + h, :] = jnp.transpose(e_scr[...])[0:1, :]

        def sweep3(kb, _):
            ps, ds = [], []
            for t in range(4):
                p = s_scr[kb, :, tile(t)] * l_scr[...]
                ps.append(p.astype(BF))
                ds.append((p * (d_scr[kb, :, tile(t)] - e_scr[...]) * SCALE).astype(BF))
            o_scr[...] += dot(jnp.concatenate(ps, axis=1), ag[kb, :, b + HB:b + HQKV])
            q_scr[...] += dot(jnp.concatenate(ds, axis=1), ag[kb, :, b + LANE:b + HB])
            return 0
        lax.fori_loop(lo, hi, sweep3, 0)
        o[:, h * LANE:(h + 1) * LANE] = o_scr[...].astype(BF)
        dq[:, h * LANE:(h + 1) * LANE] = q_scr[...].astype(BF)


def attend_t(cuts, ag, sg, dq, out, k_scr, v_scr):
    r = lax.axis_index('row')
    c1, c2 = cuts[0], cuts[1]
    lo, hi = bounds(r, c1, c2)
    kdoc = doc_of(r * SB + lax.broadcasted_iota(jnp.int32, (SB, LANE), 0), c1, c2)
    for h in range(2):
        b = h * HQKV
        k_scr[...] = jnp.zeros_like(k_scr)
        v_scr[...] = jnp.zeros_like(v_scr)

        def sweep(qb, _):
            q, do = ag[qb, :, b:b + LANE], ag[qb, :, QKV + h * LANE:896 + h * LANE]
            s = dot(ag[r, :, b + LANE:b + HB], q, NT) * SCALE
            d = dot(ag[r, :, b + HB:b + HQKV], do, NT)
            ps, ds = [], []
            for t in range(4):
                qdoc = doc_of(qb * SB + t * LANE + lax.broadcasted_iota(jnp.int32, (1, LANE), 1), c1, c2)
                v = s[:, tile(t)] - sg[qb, h:h + 1, tile(t)]
                p = jnp.exp(jnp.where(kdoc == qdoc, v, -jnp.inf))
                ps.append(p.astype(BF))
                ds.append((p * (d[:, tile(t)] - sg[qb, 2 + h:3 + h, tile(t)]) * SCALE).astype(BF))
            v_scr[...] += dot(jnp.concatenate(ps, axis=1), do)
            k_scr[...] += dot(jnp.concatenate(ds, axis=1), q)
            return 0
        lax.fori_loop(lo, hi, sweep, 0)
        out[:, b:b + LANE] = dq[:, h * LANE:(h + 1) * LANE]
        out[:, b + LANE:b + HB] = k_scr[...].astype(BF)
        out[:, b + HB:b + HQKV] = v_scr[...].astype(BF)


def weight_grad(xt, dq, out, acc):
    i = pl.program_id(0)

    @pl.when(i == 0)
    def _():
        acc[...] = jnp.zeros_like(acc)

    for k in range(2):
        acc[pl.ds(k * HB, HB), :] += (dot(xt[0, k], dq[0, pl.ds(0, HB), :], TN)
                                        + dot(xt[1, k], dq[0, pl.ds(HB, HB), :], TN))

    @pl.when(i == NR - 1)
    def _():
        out[...] = acc[...].astype(BF)


def out_grad(og, dyt, out, acc):
    i = pl.program_id(0)

    @pl.when(i == 0)
    def _():
        acc[...] = jnp.zeros_like(acc)

    for k in range(2):
        acc[k] += (dot(og[0, pl.ds(0, HB), :], dyt[0, k], TN)
                   + dot(og[0, pl.ds(HB, HB), :], dyt[1, k], TN))

    @pl.when(i == NR - 1)
    def _():
        out[...] = acc[...].astype(BF)


def vm():
    return pl.BlockSpec(memory_space=pltpu.VMEM)


def hb():
    return pl.BlockSpec(memory_space=pl.ANY)


def sds(shape, dtype=BF):
    return jax.ShapeDtypeStruct(shape, dtype)


def net_call(fn, args, outs, cid, copies, n_local, scratch=(), out_specs=None):
    return pl.pallas_call(
        fn, out_shape=outs, in_specs=[vm()] * len(args),
        out_specs=out_specs or [hb()] * len(outs),
        scratch_shapes=[*scratch, pltpu.SemaphoreType.DMA((copies,)), pltpu.SemaphoreType.DMA((copies,)),
                        pltpu.SemaphoreType.DMA((n_local,))],
        compiler_params=pltpu.CompilerParams(collective_id=cid, has_side_effects=True, vmem_limit_bytes=VLIM),
    )(*args)


def core_call(fn, args, out, scratch):
    specs = [pl.BlockSpec(memory_space=pltpu.SMEM)] + [vm()] * (len(args) - 1)
    return pl.pallas_call(
        fn, out_shape=out, in_specs=specs, out_specs=jax.tree.map(lambda _: vm(), out),
        scratch_shapes=scratch, compiler_params=pltpu.CompilerParams(vmem_limit_bytes=VLIM))(*args)


def step_call(fn, args, blocks, out, scratch):
    def spec(b):
        return pl.BlockSpec(b, lambda i, n=len(b): (i,) + (0,) * (n - 1))
    return pl.pallas_call(
        fn, grid=(NR,), out_shape=out, in_specs=[spec(b) for b in blocks],
        out_specs=pl.BlockSpec(out.shape, lambda i, n=len(out.shape): (0,) * n),
        scratch_shapes=scratch, compiler_params=pltpu.CompilerParams(vmem_limit_bytes=VLIM))(*args)


def grad_step(x_blk, wqkv_blk, wout_blk, seg_blk, dy_blk):
    x3, dy3, wo3 = (a.reshape(2, HB, HB) for a in (x_blk, dy_blk, wout_blk))
    seg8 = jnp.concatenate([seg_blk, seg_blk]).reshape(8, LANE)
    plane = (4, 4, 2, HB, HB)
    piece = (2, HB, HB)
    xg, dyg, wg, wog, segg, xt, dyt, _ = net_call(
        gather_in, (x3, dy3, wqkv_blk, wo3, seg8),
        (sds(plane), sds(plane), sds((NR, SB, QKV)), sds((NR,) + piece), sds((NR, 8, LANE), jnp.int32),
         sds(piece), sds(piece), sds(piece)),
        cid=1, copies=64, n_local=7, out_specs=[hb()] * 5 + [vm()] * 3)
    cuts = jnp.stack([jnp.sum(segg[:, :4] < 1, dtype=jnp.int32), jnp.sum(segg[:, :4] < 2, dtype=jnp.int32)])
    pair = (2, 2, HB, HB)
    qkvo = step_call(
        project, (xg.reshape((NC,) + piece), wg, dyg.reshape((NC,) + piece), wog),
        (pair, (1, SB, QKV), pair, (1,) + piece), sds((SB, 1024)),
        [pltpu.VMEM((SB, QKV), F32), pltpu.VMEM((SB, HB), F32)])
    ag, xtg, dytg = net_call(
        gather_mid, (qkvo, xt, dyt), (sds((NR, SB, 1024)), sds(plane), sds(plane)), cid=2, copies=48, n_local=5)
    row128 = pltpu.VMEM((SB, LANE), F32)
    o, dq, st = core_call(
        attend, (cuts, ag), (sds((SB, HB)), sds((SB, HB)), sds((8, SB), F32)),
        [pltpu.VMEM((NR, SB, SB), F32), pltpu.VMEM((NR, SB, SB), F32)] + [row128] * 5)
    og, sg = net_call(gather_out, (o, st), (sds((NR, SB, HB)), sds((NR, 8, SB), F32)), cid=3, copies=16, n_local=2)
    dqkv = core_call(attend_t, (cuts, ag, sg, dq), sds((SB, QKV)), [row128] * 2)
    dwo = step_call(out_grad, (og, dytg.reshape((NC,) + piece)), ((1, SB, HB), pair), sds(piece),
                    [pltpu.VMEM(piece, F32)])
    b2 = pltpu.VMEM((2, 2, HB, HB), F32)
    b4 = pltpu.VMEM((2, 4, HB, HB), F32)
    bufs = [b2, b2, b4, b4, pltpu.VMEM((4, HB, HB), F32), pltpu.VMEM((2, LANE, HB), F32), pltpu.VMEM((2, HB, HB), F32)]
    dx, dqg, dwt = net_call(
        scatter_out, (dqkv, wg, dwo), (sds(piece), sds((NR, SB, QKV)), sds(piece)),
        cid=4, copies=32, n_local=1, scratch=bufs * 2, out_specs=[vm(), hb(), vm()])
    dw = step_call(weight_grad, (xtg.reshape((NC,) + piece), dqg), (pair, (1, SB, QKV)), sds((SB, QKV)),
                   [pltpu.VMEM((SB, QKV), F32)])
    return dx.reshape(SB, HB), dw, dwt.reshape(SB, HB)


def solution(mesh):
    tok_spec = P(('dp', 'row'), 'col')
    mat_spec = P('row', 'col')
    seg_spec = P(('dp', 'row'))
    return jax.shard_map(grad_step, mesh=mesh, in_specs=(tok_spec, mat_spec, mat_spec, seg_spec, tok_spec),
                         out_specs=(tok_spec, tok_spec, tok_spec), check_vma=False)
```

```python
import jax
import jax.numpy as jnp
from jax import lax
from jax.experimental import pallas as pl
from jax.experimental.pallas import tpu as pltpu
from jax.sharding import PartitionSpec as P

HEAD_DIM = 128
NR, NC = 8, 16
SB = 512
SCALE = HEAD_DIM ** -0.5
HB, LANE, QKV, HQKV = 256, 128, 768, 384
TOK = 32
MESH = pl.DeviceIdType.MESH
BF = jnp.bfloat16
F32 = jnp.float32
NT = (((1,), (1,)), ((), ()))
TN = (((0,), (0,)), ((), ()))
VLIM = 60 * 1024 * 1024


def dot(a, b, dims=None):
    if dims is None:
        dims = (((1,), (0,)), ((), ()))
    return lax.dot_general(a, b, dims, preferred_element_type=F32)


class Net:
    def __init__(self, send, recv):
        self.send, self.recv, self.n = send, recv, 0
        self.c, self.r = lax.axis_index('col'), lax.axis_index('row')
        self.x, self.core = self.r // 2, self.r % 2
        self.z, self.y = self.c // 4, self.c % 4
        self.sent = []

    def dev(self, axis, step):
        x, z, y, core = self.x, self.z, self.y, self.core
        if axis == 'x':
            x = (x + step) % 4
        elif axis == 'z':
            z = (z + step) % 4
        elif axis == 'y':
            y = (y + step) % 4
        else:
            core = 1 - core
        return {'col': z * 4 + y, 'row': x * 2 + core}

    def mate(self, k):
        return {'col': self.c, 'row': (self.r + k) % NR}

    def copy(self, src, dst, dev):
        i = self.n
        self.n += 1
        cp = pltpu.make_async_remote_copy(
            src_ref=src, dst_ref=dst, send_sem=self.send.at[i], recv_sem=self.recv.at[i],
            device_id=dev, device_id_type=MESH)
        cp.start()
        self.sent.append(cp)
        return cp

    def enter(self, axes, swap):
        bar = pltpu.get_barrier_semaphore()
        peers = []
        for a in axes:
            if a == 'row':
                peers += [self.mate(k) for k in range(1, NR)]
            else:
                peers += [self.dev(a, 1), self.dev(a, 3)] if a != 'core' else [self.dev(a, 1)]
        for d in peers:
            pl.semaphore_signal(bar, inc=1, device_id=d, device_id_type=MESH)
        if swap:
            for k in range(2):
                @pl.when(jnp.logical_not(self.own_swap(k)))
                def _():
                    pl.semaphore_signal(bar, inc=1, device_id=self.swap_dev(k), device_id_type=MESH)
            n = len(peers) + 2 - (self.c // 2 == self.r).astype(jnp.int32)
            pl.semaphore_wait(bar, n)
        else:
            pl.semaphore_wait(bar, len(peers))

    def own_swap(self, k):
        return jnp.logical_and(self.c // 2 == self.r, self.c % 2 == k)

    def swap_dev(self, k):
        return {'col': 2 * self.r + k, 'row': self.c // 2}

    def finish(self):
        for cp in self.sent:
            cp.wait_send()


def swap_steps(net, src, dst, base):
    i = net.c % 2

    def cp(k, slot):
        return pltpu.make_async_remote_copy(
            src_ref=src.at[k], dst_ref=dst.at[slot], send_sem=net.send.at[base + k],
            recv_sem=net.recv.at[base + slot], device_id=net.swap_dev(k), device_id_type=MESH)

    for k in range(2):
        own = net.own_swap(k)

        @pl.when(jnp.logical_not(own))
        def _():
            cp(k, i).start()

        @pl.when(own)
        def _():
            dst[k] = src[k]
    yield
    for k in range(2):
        @pl.when(jnp.logical_not(net.own_swap(k)))
        def _():
            cp(k, k).wait_recv()
    net.tail.append(lambda: [pl.when(jnp.logical_not(net.own_swap(k)))(lambda k=k: cp(k, k).wait_send()) for k in range(2)])


def row_steps(net, src, out, half, local):
    x, core = net.x, net.core
    slot = lambda s: out.at[((x + s) % 4) * 2 + core]
    me = out.at[net.r]
    right, left, mate = net.dev('x', 1), net.dev('x', 3), net.dev('core', 1)
    a = net.copy(src, me, right)
    b = net.copy(src, me, left)
    got = [net.copy(src, me, mate)]
    if local is None:
        me[...] = src[...]
    else:
        own = pltpu.make_async_copy(src, me, local)
        own.start()
    yield
    a.wait_recv()
    c = net.copy(half(slot(3), 0), half(slot(3), 0), right)
    got.append(net.copy(slot(3), slot(3), mate))
    b.wait_recv()
    d = net.copy(half(slot(1), 1), half(slot(1), 1), left)
    got.append(net.copy(slot(1), slot(1), mate))
    yield
    c.wait_recv()
    d.wait_recv()
    got.append(net.copy(slot(2), slot(2), mate))
    yield
    for g in got:
        g.wait_recv()
    if local is not None:
        own.wait()


def col_steps(net, src, out, h, n, local=None):
    first, second = ('y', 'z') if h == 0 else ('z', 'y')
    z, y = net.z, net.y

    def one(s):
        return out.at[z, (y + s) % 4, h] if h == 0 else out.at[(z + s) % 4, y, h]

    def four(s):
        return out.at[(z + s) % 4, pl.ds(0, 4), h] if h == 0 else out.at[pl.ds(0, 4), (y + s) % 4, h]

    def pair(s, k):
        return out.at[(z + s) % 4, pl.ds(2 * k, 2), h] if h == 0 else out.at[pl.ds(2 * k, 2), (y + s) % 4, h]

    def rows(ref, k):
        return ref.at[pl.ds(k * n, n)]

    right, left = net.dev(first, 1), net.dev(first, 3)
    a = net.copy(src.at[h], one(0), right)
    b = net.copy(src.at[h], one(0), left)
    if local is None:
        one(0)[...] = src[h]
    else:
        own = pltpu.make_async_copy(src.at[h], one(0), local)
        own.start()
    yield
    a.wait_recv()
    c = net.copy(rows(one(3), 0), rows(one(3), 0), right)
    b.wait_recv()
    d = net.copy(rows(one(1), 1), rows(one(1), 1), left)
    yield
    if local is not None:
        own.wait()
    c.wait_recv()
    d.wait_recv()
    right, left = net.dev(second, 1), net.dev(second, 3)
    a = net.copy(four(0), four(0), right)
    b = net.copy(four(0), four(0), left)
    yield
    a.wait_recv()
    c = net.copy(pair(3, 0), pair(3, 0), right)
    b.wait_recv()
    d = net.copy(pair(1, 1), pair(1, 1), left)
    yield
    c.wait_recv()
    d.wait_recv()


def half_rows(n):
    return lambda ref, h: ref.at[pl.ds(h * n, n)]


def half_lead(ref, h):
    return ref.at[h]


def exchange(net, full, part):
    lead, off = net.c // NR, pl.multiple_of((net.c % NR) * TOK, TOK)

    def piece(r):
        return full.at[r // 2, pl.ds((r % 2) * 2, 2), lead, pl.ds(off, TOK)]

    mine = part.at[net.r // 4, net.r % 4]
    got = []
    for k in range(1, NR):
        got.append(net.copy(piece((net.r + k) % NR), mine, net.mate(k)))
    part[net.r // 4, net.r % 4] = piece(net.r)[...]
    yield
    for g in got:
        g.wait_recv()


def front(x, dy, w, wo, seg, segg, wout, ag, ado, xtg, dytg,
          xg, dyg, wg, wog, wot, xt, dyt, acc, qkv, do, send, recv, local):
    net = Net(send, recv)
    net.tail = []
    net.enter(('row', 'z', 'y'), True)
    net.n = 2

    def both(src, out, n, loc=(None, None)):
        g = [col_steps(net, src, out, h, n, loc[h]) for h in range(2)]
        for _ in range(5):
            for a in g:
                next(a, None)
            yield

    def go(*gens):
        for g in gens:
            next(g, None)

    gx, gdy = both(x, xg, LANE), both(dy, dyg, LANE)
    gw = row_steps(net, w, wg, half_rows(HB), None)
    gs = row_steps(net, seg, segg, half_rows(4), local.at[0])
    gsw = swap_steps(net, wo, wot, 0)
    gwo = row_steps(net, wot, wog, half_lead, None)
    ex, ey = exchange(net, xg, xt), exchange(net, dyg, dyt)
    gxt = both(xt, xtg, 2, (local.at[1], local.at[2]))
    gdyt = both(dyt, dytg, 2, (local.at[3], local.at[4]))
    gq = row_steps(net, qkv, ag, half_rows(HB), local.at[5])
    gdo = row_steps(net, do, ado, half_rows(HB), local.at[6])

    go(gx, gs, gw, gsw, gx, gx, gdy, gsw, gs, gw, gwo, gs, gx, gdy, gw, gs, gw, gx, gdy, ex)
    keep = pltpu.make_async_copy(wg, wout, local.at[7])
    keep.start()
    go(gwo)

    def qkv_step(c, a):
        xb = xg[c // 4, c % 4].reshape(SB, HB)
        wb = wg[c // 2, pl.ds(pl.multiple_of((c % 2) * HB, HB), HB), :]
        acc[...] += dot(xb, wb)
        return a
    acc[...] = jnp.zeros_like(acc)
    lax.fori_loop(0, NC, qkv_step, 0)
    qkv[...] = acc[...].astype(BF)
    go(gwo, ex, gq, gxt, gwo, gdy, gxt, gdy, ey)

    def do_step(c, a):
        yb = dyg[c // 4, c % 4].reshape(SB, HB)
        acc[:, pl.ds(0, HB)] += dot(yb, wog[c // 2, c % 2], NT)
        return a
    acc[...] = jnp.zeros_like(acc)
    lax.fori_loop(0, NC, do_step, 0)
    do[...] = acc[:, pl.ds(0, HB)].astype(BF)
    go(ey, gxt, gdo, gdyt, gq, gdyt, gdo, gxt, gq, gdo, gxt, gdyt, gq, gdo, gdyt, gdyt)
    keep.wait()
    for g in (gx, gdy, gw, gs, gsw, gwo, ex, ey, gxt, gdyt, gq, gdo):
        for _ in g:
            pass
    net.finish()
    for f in net.tail:
        f()


def share(st, sg, send, recv, local):
    net = Net(send, recv)
    net.tail = []
    net.enter(('row',), False)
    mine = sg.at[net.r]
    own = pltpu.make_async_copy(st, mine, local.at[0])
    own.start()
    got = [net.copy(st, mine, net.mate(k)) for k in range(1, NR)]
    own.wait()
    for g in got:
        g.wait_recv()
    net.finish()


def scatter_steps(net, h, dq, w, dx, s1, r1, s2, r2, own, r3, r4):
    first, second = ('z', 'y') if h == 0 else ('y', 'z')
    f, g = (net.z, net.y) if h == 0 else (net.y, net.z)

    def part(ft, gt):
        c = ft * 4 + gt if h == 0 else gt * 4 + ft
        wb = w[c // 2, pl.ds(pl.multiple_of((c % 2) * HB, HB), HB), :]
        return dot(dq[pl.ds(h * HB, HB), :], wb, NT)

    def fill(dst, ft, base):
        def body(j, _):
            dst[j] = part(ft, base + j)
            return 0
        lax.fori_loop(0, dst.shape[0], body, 0)

    right, left = net.dev(first, 1), net.dev(first, 3)
    fill(s1.at[0], (f + 2) % 4, 0)
    fill(s1.at[1], (f + 2) % 4, 2)
    a = net.copy(s1.at[0], r1.at[0], right)
    b = net.copy(s1.at[1], r1.at[1], left)
    yield
    fill(s2.at[0], (f + 1) % 4, 0)
    a2 = net.copy(s2.at[0, pl.ds(2, 2)], r2.at[0, pl.ds(2, 2)], right)
    fill(s2.at[1], (f + 3) % 4, 0)
    b2 = net.copy(s2.at[1, pl.ds(0, 2)], r2.at[1, pl.ds(0, 2)], left)
    yield
    a.wait_recv()

    def add0(j, _):
        s2[0, j] = s2[0, j] + r1[0, j]
        return 0
    lax.fori_loop(0, 2, add0, 0)
    b.wait_recv()

    def add1(j, _):
        s2[1, 2 + j] = s2[1, 2 + j] + r1[1, j]
        return 0
    lax.fori_loop(0, 2, add1, 0)
    a = net.copy(s2.at[0, pl.ds(0, 2)], r2.at[0, pl.ds(0, 2)], right)
    b = net.copy(s2.at[1, pl.ds(2, 2)], r2.at[1, pl.ds(2, 2)], left)
    fill(own, f, 0)
    yield
    for cp in (a2, b2, a, b):
        cp.wait_recv()

    def add2(j, _):
        own[j] = own[j] + r2[0, j] + r2[1, j]
        return 0
    lax.fori_loop(0, 4, add2, 0)
    right, left = net.dev(second, 1), net.dev(second, 3)
    go, gr, gl = (g + 2) % 4, (g + 1) % 4, (g + 3) % 4
    up, low = pl.ds(0, LANE), pl.ds(LANE, LANE)
    a = net.copy(own.at[go, up], r3.at[0], right)
    b = net.copy(own.at[go, low], r3.at[1], left)
    a2 = net.copy(own.at[gr, low], r4.at[0, low], right)
    b2 = net.copy(own.at[gl, up], r4.at[1, up], left)
    yield
    a.wait_recv()
    own[gr, up, :] = own[gr, up, :] + r3[0]
    b.wait_recv()
    own[gl, low, :] = own[gl, low, :] + r3[1]
    a = net.copy(own.at[gr, up], r4.at[0, up], right)
    b = net.copy(own.at[gl, low], r4.at[1, low], left)
    yield
    for cp in (a2, b2, a, b):
        cp.wait_recv()
    dx[h] = (own[g] + r4[0] + r4[1]).astype(BF)


def back(dq, o, wg, xtg, dytg, dx, dw, dwt, *scr):
    bufs, (w, xt, dyt, og, dqg, acc, acco, dwo, send, recv, local) = scr[:14], scr[14:]
    loads = [pltpu.make_async_copy(a, b, local.at[i]) for i, (a, b) in enumerate(((wg, w), (dytg, dyt), (xtg, xt)))]
    for cp in loads:
        cp.start()
    net = Net(send, recv)
    net.tail = []
    net.enter(('x', 'z', 'y', 'core'), True)
    net.n = 2

    def go(*gens):
        for g in gens:
            next(g, None)

    gog = row_steps(net, o, og, half_rows(HB), None)
    gdq = row_steps(net, dq, dqg, half_rows(HB), None)
    rs0 = scatter_steps(net, 0, dq, w, dx, *bufs[:7])
    rs1 = scatter_steps(net, 1, dq, w, dx, *bufs[7:])
    gsw = swap_steps(net, dwo, dwt, 0)
    go(gog, gdq)
    loads[0].wait()
    go(rs0, rs1, rs0, rs1, gog, rs0, rs1, gog, gog)
    loads[1].wait()

    def tokens(ref, r, k):
        return ref[:, :, r // 4, r % 4, k].reshape(SB, HB)

    def dwo_step(r, a):
        for k in range(2):
            acco[k] += dot(og[r], tokens(dyt, r, k), TN)
        return a
    acco[...] = jnp.zeros_like(acco)
    lax.fori_loop(0, NR, dwo_step, 0)
    dwo[...] = acco[...].astype(BF)
    go(gdq, gsw, gdq, gdq)
    loads[2].wait()

    def dw_step(r, a):
        for k in range(2):
            acc[pl.ds(k * HB, HB), :] += dot(tokens(xt, r, k), dqg[r], TN)
        return a
    acc[...] = jnp.zeros_like(acc)
    lax.fori_loop(0, NR, dw_step, 0)
    go(rs0, rs1, rs0, rs1)
    dw[...] = acc[...].astype(BF)
    go(rs0, rs1, gsw)
    for g in (gog, gdq, rs0, rs1, gsw):
        for _ in g:
            pass
    net.finish()
    for f in net.tail:
        f()


def doc_of(pos, c1, c2):
    return (pos >= c1).astype(jnp.int32) + (pos >= c2).astype(jnp.int32)


def bounds(r, c1, c2):
    p0, p1 = r * SB, r * SB + SB - 1
    lo = jnp.where(p0 >= c2, c2, jnp.where(p0 >= c1, c1, 0))
    hi = jnp.where(p1 >= c2, NR * SB, jnp.where(p1 >= c1, c2, c1))
    return lo // SB, (hi + SB - 1) // SB


def cuts_of(seg):
    return [jnp.sum((seg[...] < d).astype(F32)).astype(jnp.int32) // 2 for d in (1, 2)]


def tile(t):
    return slice(t * LANE, (t + 1) * LANE)


def attend(seg, ag, ado, o, dq, st, s_scr, d_scr, m_scr, l_scr, e_scr, o_scr, q_scr):
    r = lax.axis_index('row')
    c1, c2 = cuts_of(seg)
    lo, hi = bounds(r, c1, c2)
    qdoc = doc_of(r * SB + lax.broadcasted_iota(jnp.int32, (SB, LANE), 0), c1, c2)
    st[...] = jnp.zeros_like(st)
    for h in range(2):
        b = h * HQKV
        m_scr[...] = jnp.full(m_scr.shape, -jnp.inf, F32)
        l_scr[...] = jnp.zeros_like(l_scr)
        e_scr[...] = jnp.zeros_like(e_scr)
        o_scr[...] = jnp.zeros_like(o_scr)
        q_scr[...] = jnp.zeros_like(q_scr)

        def sweep1(kb, _):
            s = dot(ag[r, :, b:b + LANE], ag[kb, :, b + LANE:b + HB], NT) * SCALE
            m = m_scr[...]
            for t in range(4):
                kdoc = doc_of(kb * SB + t * LANE + lax.broadcasted_iota(jnp.int32, (1, LANE), 1), c1, c2)
                v = jnp.where(qdoc == kdoc, s[:, tile(t)], -jnp.inf)
                s_scr[kb, :, tile(t)] = v
                m = jnp.maximum(m, v)
            m_scr[...] = m
            return 0
        lax.fori_loop(lo, hi, sweep1, 0)
        m_scr[...] = jnp.broadcast_to(jnp.max(m_scr[...], axis=1, keepdims=True), m_scr.shape)

        def sweep2(kb, _):
            d = dot(ado[r, :, h * LANE:(h + 1) * LANE], ag[kb, :, b + HB:b + HQKV], NT)
            l, e, m = l_scr[...], e_scr[...], m_scr[...]
            for t in range(4):
                p = jnp.exp(s_scr[kb, :, tile(t)] - m)
                s_scr[kb, :, tile(t)] = p
                d_scr[kb, :, tile(t)] = d[:, tile(t)]
                l = l + p
                e = e + p * d[:, tile(t)]
            l_scr[...] = l
            e_scr[...] = e
            return 0
        lax.fori_loop(lo, hi, sweep2, 0)
        tot = jnp.sum(l_scr[...], axis=1, keepdims=True)
        dot_row = jnp.sum(e_scr[...], axis=1, keepdims=True) / tot
        lse = jnp.broadcast_to(m_scr[:, 0:1] + jnp.log(tot), m_scr.shape)
        st[h:h + 1, :] = jnp.transpose(lse)[0:1, :]
        l_scr[...] = jnp.broadcast_to(1.0 / tot, l_scr.shape)
        e_scr[...] = jnp.broadcast_to(dot_row, e_scr.shape)
        st[2 + h:3 + h, :] = jnp.transpose(e_scr[...])[0:1, :]

        def sweep3(kb, _):
            ps, ds = [], []
            for t in range(4):
                p = s_scr[kb, :, tile(t)] * l_scr[...]
                ps.append(p.astype(BF))
                ds.append((p * (d_scr[kb, :, tile(t)] - e_scr[...]) * SCALE).astype(BF))
            o_scr[...] += dot(jnp.concatenate(ps, axis=1), ag[kb, :, b + HB:b + HQKV])
            q_scr[...] += dot(jnp.concatenate(ds, axis=1), ag[kb, :, b + LANE:b + HB])
            return 0
        lax.fori_loop(lo, hi, sweep3, 0)
        o[:, h * LANE:(h + 1) * LANE] = o_scr[...].astype(BF)
        dq[:, h * LANE:(h + 1) * LANE] = q_scr[...].astype(BF)


def attend_t(seg, ag, ado, sg, dq, out, k_scr, v_scr):
    r = lax.axis_index('row')
    c1, c2 = cuts_of(seg)
    lo, hi = bounds(r, c1, c2)
    kdoc = doc_of(r * SB + lax.broadcasted_iota(jnp.int32, (SB, LANE), 0), c1, c2)
    for h in range(2):
        b = h * HQKV
        k_scr[...] = jnp.zeros_like(k_scr)
        v_scr[...] = jnp.zeros_like(v_scr)

        def sweep(qb, _):
            q, do = ag[qb, :, b:b + LANE], ado[qb, :, h * LANE:(h + 1) * LANE]
            s = dot(ag[r, :, b + LANE:b + HB], q, NT) * SCALE
            d = dot(ag[r, :, b + HB:b + HQKV], do, NT)
            ps, ds = [], []
            for t in range(4):
                qdoc = doc_of(qb * SB + t * LANE + lax.broadcasted_iota(jnp.int32, (1, LANE), 1), c1, c2)
                v = s[:, tile(t)] - sg[qb, h:h + 1, tile(t)]
                p = jnp.exp(jnp.where(kdoc == qdoc, v, -jnp.inf))
                ps.append(p.astype(BF))
                ds.append((p * (d[:, tile(t)] - sg[qb, 2 + h:3 + h, tile(t)]) * SCALE).astype(BF))
            v_scr[...] += dot(jnp.concatenate(ps, axis=1), do)
            k_scr[...] += dot(jnp.concatenate(ds, axis=1), q)
            return 0
        lax.fori_loop(lo, hi, sweep, 0)
        out[:, b:b + LANE] = dq[:, h * LANE:(h + 1) * LANE]
        out[:, b + LANE:b + HB] = k_scr[...].astype(BF)
        out[:, b + HB:b + HQKV] = v_scr[...].astype(BF)


def vm():
    return pl.BlockSpec(memory_space=pltpu.VMEM)


def hb():
    return pl.BlockSpec(memory_space=pl.ANY)


def sds(shape, dtype=BF):
    return jax.ShapeDtypeStruct(shape, dtype)


def net_call(fn, args, outs, cid, copies, n_local, scratch=(), out_specs=None, in_specs=None):
    return pl.pallas_call(
        fn, out_shape=outs, in_specs=in_specs or [vm()] * len(args),
        out_specs=out_specs or [hb()] * len(outs),
        scratch_shapes=[*scratch, pltpu.SemaphoreType.DMA((copies,)), pltpu.SemaphoreType.DMA((copies,)),
                        pltpu.SemaphoreType.DMA((n_local,))],
        compiler_params=pltpu.CompilerParams(collective_id=cid, has_side_effects=True, vmem_limit_bytes=VLIM),
    )(*args)


def core_call(fn, args, out, scratch):
    specs = [vm()] * len(args)
    return pl.pallas_call(
        fn, out_shape=out, in_specs=specs, out_specs=jax.tree.map(lambda _: vm(), out),
        scratch_shapes=scratch, compiler_params=pltpu.CompilerParams(vmem_limit_bytes=VLIM))(*args)


def grad_step(x_blk, wqkv_blk, wout_blk, seg_blk, dy_blk):
    x3, dy3, wo3 = (a.reshape(2, HB, HB) for a in (x_blk, dy_blk, wout_blk))
    seg8 = jnp.concatenate([seg_blk, seg_blk]).reshape(8, LANE)
    piece = (2, HB, HB)
    part = (2, 4, 2, TOK, HB)
    gathered = (NC, NR, 2, TOK, HB)
    plane = pltpu.VMEM((4, 4) + piece, BF)
    segg, wg, ag, ado, xtg, dytg = net_call(
        front, (x3, dy3, wqkv_blk, wo3, seg8),
        (sds((NR, 8, LANE), jnp.int32), sds((NR, SB, QKV)), sds((NR, SB, QKV)), sds((NR, SB, HB)),
         sds((4, 4) + part), sds((4, 4) + part)),
        cid=1, copies=120, n_local=8,
        scratch=[plane, plane, pltpu.VMEM((NR, SB, QKV), BF), pltpu.VMEM((NR,) + piece, BF), pltpu.VMEM(piece, BF),
                 pltpu.VMEM(part, BF), pltpu.VMEM(part, BF), pltpu.VMEM((SB, QKV), F32),
                 pltpu.VMEM((SB, QKV), BF), pltpu.VMEM((SB, HB), BF)])
    row128 = pltpu.VMEM((SB, LANE), F32)
    o, dq, st = core_call(
        attend, (segg, ag, ado), (sds((SB, HB)), sds((SB, HB)), sds((8, SB), F32)),
        [pltpu.VMEM((NR, SB, SB), F32), pltpu.VMEM((NR, SB, SB), F32)] + [row128] * 5)
    sg, = net_call(share, (st,), (sds((NR, 8, SB), F32),), cid=3, copies=7, n_local=1)
    dqkv = core_call(attend_t, (segg, ag, ado, sg, dq), sds((SB, QKV)), [row128] * 2)
    b2, b4 = pltpu.VMEM((2,) + piece, F32), pltpu.VMEM((2, 4, HB, HB), F32)
    bufs = [b2, b2, b4, b4, pltpu.VMEM((4, HB, HB), F32), pltpu.VMEM((2, LANE, HB), F32), pltpu.VMEM(piece, F32)]
    tokens = pltpu.VMEM((4, 4) + part, BF)
    dx, dw, dwt = net_call(
        back, (dqkv, o, wg, xtg, dytg), (sds(piece), sds((SB, QKV)), sds(piece)), cid=4, copies=42, n_local=3,
        scratch=bufs * 2 + [pltpu.VMEM((NR, SB, QKV), BF), tokens, tokens, pltpu.VMEM((NR, SB, HB), BF),
                            pltpu.VMEM((NR, SB, QKV), BF), pltpu.VMEM((SB, QKV), F32), pltpu.VMEM(piece, F32),
                            pltpu.VMEM(piece, BF)],
        in_specs=[vm()] * 2 + [hb()] * 3, out_specs=[vm()] * 3)
    return dx.reshape(SB, HB), dw, dwt.reshape(SB, HB)


def solution(mesh):
    tok_spec = P(('dp', 'row'), 'col')
    mat_spec = P('row', 'col')
    seg_spec = P(('dp', 'row'))
    return jax.shard_map(grad_step, mesh=mesh, in_specs=(tok_spec, mat_spec, mat_spec, seg_spec, tok_spec),
                         out_specs=(tok_spec, tok_spec, tok_spec), check_vma=False)
```

```python
import jax
import jax.numpy as jnp
from jax import lax
from jax.experimental import pallas as pl
from jax.experimental.pallas import tpu as pltpu
from jax.sharding import PartitionSpec as P

HEAD_DIM = 128
NR, NC = 8, 16
SB = 512
SCALE = HEAD_DIM ** -0.5
HB, LANE, QKV, HQKV = 256, 128, 768, 384
TOK = 32
MESH = pl.DeviceIdType.MESH
BF = jnp.bfloat16
F32 = jnp.float32
NT = (((1,), (1,)), ((), ()))
TN = (((0,), (0,)), ((), ()))
VLIM = 60 * 1024 * 1024


def dot(a, b, dims=None):
    if dims is None:
        dims = (((1,), (0,)), ((), ()))
    return lax.dot_general(a, b, dims, preferred_element_type=F32)


class Net:
    def __init__(self, send, recv):
        self.send, self.recv, self.n = send, recv, 0
        self.c, self.r = lax.axis_index('col'), lax.axis_index('row')
        self.x, self.core = self.r // 2, self.r % 2
        self.z, self.y = self.c // 4, self.c % 4
        self.sent = []

    def dev(self, axis, step):
        x, z, y, core = self.x, self.z, self.y, self.core
        if axis == 'x':
            x = (x + step) % 4
        elif axis == 'z':
            z = (z + step) % 4
        elif axis == 'y':
            y = (y + step) % 4
        else:
            core = 1 - core
        return {'col': z * 4 + y, 'row': x * 2 + core}

    def mate(self, k):
        return {'col': self.c, 'row': (self.r + k) % NR}

    def copy(self, src, dst, dev):
        i = self.n
        self.n += 1
        cp = pltpu.make_async_remote_copy(
            src_ref=src, dst_ref=dst, send_sem=self.send.at[i], recv_sem=self.recv.at[i],
            device_id=dev, device_id_type=MESH)
        cp.start()
        self.sent.append(cp)
        return cp

    def enter(self, axes, swap):
        bar = pltpu.get_barrier_semaphore()
        peers = []
        for a in axes:
            if a == 'row':
                peers += [self.mate(k) for k in range(1, NR)]
            else:
                peers += [self.dev(a, 1), self.dev(a, 3)] if a != 'core' else [self.dev(a, 1)]
        for d in peers:
            pl.semaphore_signal(bar, inc=1, device_id=d, device_id_type=MESH)
        if swap:
            for k in range(2):
                @pl.when(jnp.logical_not(self.own_swap(k)))
                def _():
                    pl.semaphore_signal(bar, inc=1, device_id=self.swap_dev(k), device_id_type=MESH)
            n = len(peers) + 2 - (self.c // 2 == self.r).astype(jnp.int32)
            pl.semaphore_wait(bar, n)
        else:
            pl.semaphore_wait(bar, len(peers))

    def own_swap(self, k):
        return jnp.logical_and(self.c // 2 == self.r, self.c % 2 == k)

    def swap_dev(self, k):
        return {'col': 2 * self.r + k, 'row': self.c // 2}

    def finish(self):
        for cp in self.sent:
            cp.wait_send()


def swap_steps(net, src, dst, base):
    i = net.c % 2

    def cp(k, slot):
        return pltpu.make_async_remote_copy(
            src_ref=src.at[k], dst_ref=dst.at[slot], send_sem=net.send.at[base + k],
            recv_sem=net.recv.at[base + slot], device_id=net.swap_dev(k), device_id_type=MESH)

    for k in range(2):
        own = net.own_swap(k)

        @pl.when(jnp.logical_not(own))
        def _():
            cp(k, i).start()

        @pl.when(own)
        def _():
            dst[k] = src[k]
    yield
    for k in range(2):
        @pl.when(jnp.logical_not(net.own_swap(k)))
        def _():
            cp(k, k).wait_recv()
    net.tail.append(lambda: [pl.when(jnp.logical_not(net.own_swap(k)))(lambda k=k: cp(k, k).wait_send()) for k in range(2)])


def row_steps(net, src, out, half, local):
    x, core = net.x, net.core
    slot = lambda s: out.at[((x + s) % 4) * 2 + core]
    me = out.at[net.r]
    right, left, mate = net.dev('x', 1), net.dev('x', 3), net.dev('core', 1)
    a = [net.copy(half(src, 0), half(me, 0), right)]
    b = [net.copy(half(src, 1), half(me, 1), left)]
    a.append(net.copy(half(src, 1), half(me, 1), right))
    b.append(net.copy(half(src, 0), half(me, 0), left))
    got = [net.copy(src, me, mate)]
    if local is None:
        me[...] = src[...]
    else:
        own = pltpu.make_async_copy(src, me, local)
        own.start()
    yield
    a[0].wait_recv()
    c = net.copy(half(slot(3), 0), half(slot(3), 0), right)
    b[0].wait_recv()
    d = net.copy(half(slot(1), 1), half(slot(1), 1), left)
    yield
    a[1].wait_recv()
    got.append(net.copy(slot(3), slot(3), mate))
    b[1].wait_recv()
    got.append(net.copy(slot(1), slot(1), mate))
    c.wait_recv()
    d.wait_recv()
    got.append(net.copy(slot(2), slot(2), mate))
    yield
    for g in got:
        g.wait_recv()
    if local is not None:
        own.wait()


def col_steps(net, src, out, h, n, local=None):
    first, second = ('y', 'z') if h == 0 else ('z', 'y')
    z, y = net.z, net.y

    def one(s):
        return out.at[z, (y + s) % 4, h] if h == 0 else out.at[(z + s) % 4, y, h]

    def pair(s, k):
        return out.at[(z + s) % 4, pl.ds(2 * k, 2), h] if h == 0 else out.at[pl.ds(2 * k, 2), (y + s) % 4, h]

    def rows(ref, k):
        return ref.at[pl.ds(k * n, n)]

    right, left = net.dev(first, 1), net.dev(first, 3)
    a = [net.copy(rows(src.at[h], 0), rows(one(0), 0), right)]
    b = [net.copy(rows(src.at[h], 1), rows(one(0), 1), left)]
    a.append(net.copy(rows(src.at[h], 1), rows(one(0), 1), right))
    b.append(net.copy(rows(src.at[h], 0), rows(one(0), 0), left))
    if local is None:
        one(0)[...] = src[h]
    else:
        own = pltpu.make_async_copy(src.at[h], one(0), local)
        own.start()
    yield
    a[0].wait_recv()
    c = net.copy(rows(one(3), 0), rows(one(3), 0), right)
    b[0].wait_recv()
    d = net.copy(rows(one(1), 1), rows(one(1), 1), left)
    yield
    if local is not None:
        own.wait()
    for cp in (a[1], b[1], c, d):
        cp.wait_recv()
    right, left = net.dev(second, 1), net.dev(second, 3)
    a = [net.copy(pair(0, 0), pair(0, 0), right)]
    b = [net.copy(pair(0, 1), pair(0, 1), left)]
    a.append(net.copy(pair(0, 1), pair(0, 1), right))
    b.append(net.copy(pair(0, 0), pair(0, 0), left))
    yield
    a[0].wait_recv()
    c = net.copy(pair(3, 0), pair(3, 0), right)
    b[0].wait_recv()
    d = net.copy(pair(1, 1), pair(1, 1), left)
    yield
    for cp in (a[1], b[1], c, d):
        cp.wait_recv()


def half_rows(n):
    return lambda ref, h: ref.at[pl.ds(h * n, n)]


def half_lead(ref, h):
    return ref.at[h]


def exchange(net, full, part):
    lead, off = net.c // NR, pl.multiple_of((net.c % NR) * TOK, TOK)

    def piece(r):
        return full.at[r // 2, pl.ds((r % 2) * 2, 2), lead, pl.ds(off, TOK)]

    mine = part.at[net.r // 4, net.r % 4]
    got = []
    for k in range(1, NR):
        got.append(net.copy(piece((net.r + k) % NR), mine, net.mate(k)))
    part[net.r // 4, net.r % 4] = piece(net.r)[...]
    yield
    for g in got:
        g.wait_recv()


def front(x, dy, w, wo, seg, segg, wout, ag, ado, xtg, dytg,
          xg, dyg, wg, wog, wot, xt, dyt, acc, qkv, do, send, recv, local):
    net = Net(send, recv)
    net.tail = []
    net.enter(('row', 'z', 'y'), True)
    net.n = 2

    def both(src, out, n, loc=(None, None)):
        g = [col_steps(net, src, out, h, n, loc[h]) for h in range(2)]
        for _ in range(5):
            for a in g:
                next(a, None)
            yield

    def go(*gens):
        for g in gens:
            next(g, None)

    gx, gdy = both(x, xg, LANE), both(dy, dyg, LANE)
    gw = row_steps(net, w, wg, half_rows(HB), None)
    gs = row_steps(net, seg, segg, half_rows(4), local.at[0])
    gsw = swap_steps(net, wo, wot, 0)
    gwo = row_steps(net, wot, wog, half_lead, None)
    ex, ey = exchange(net, xg, xt), exchange(net, dyg, dyt)
    gxt = both(xt, xtg, 2, (local.at[1], local.at[2]))
    gdyt = both(dyt, dytg, 2, (local.at[3], local.at[4]))
    gq = row_steps(net, qkv, ag, half_rows(HB), local.at[5])
    gdo = row_steps(net, do, ado, half_rows(HB), local.at[6])

    go(gx, gs, gdy, gsw, gw, gx, gx, gdy, gsw, gs, gw, gwo, gx, gdy, gs, gx, ex, gw, gs, gw)
    keep = pltpu.make_async_copy(wg, wout, local.at[7])
    keep.start()
    go(gwo)

    def qkv_step(c, a):
        xb = xg[c // 4, c % 4].reshape(SB, HB)
        wb = wg[c // 2, pl.ds(pl.multiple_of((c % 2) * HB, HB), HB), :]
        acc[...] += dot(xb, wb)
        return a
    acc[...] = jnp.zeros_like(acc)
    lax.fori_loop(0, NC, qkv_step, 0)
    qkv[...] = acc[...].astype(BF)
    go(gq, gdy, ex, gxt, gwo, gwo, gdy, ey)

    def do_step(c, a):
        yb = dyg[c // 4, c % 4].reshape(SB, HB)
        acc[:, pl.ds(0, HB)] += dot(yb, wog[c // 2, c % 2], NT)
        return a
    acc[...] = jnp.zeros_like(acc)
    lax.fori_loop(0, NC, do_step, 0)
    do[...] = acc[:, pl.ds(0, HB)].astype(BF)
    go(gdo, gxt, gxt, ey, gdyt, gq, gxt, gdyt, gdyt, gdo, gxt, gq, gdo, gdyt, gq, gdo, gdyt)
    keep.wait()
    for g in (gx, gdy, gw, gs, gsw, gwo, ex, ey, gxt, gdyt, gq, gdo):
        for _ in g:
            pass
    net.finish()
    for f in net.tail:
        f()


def share(st, sg, send, recv, local):
    net = Net(send, recv)
    net.tail = []
    net.enter(('row',), False)
    mine = sg.at[net.r]
    own = pltpu.make_async_copy(st, mine, local.at[0])
    own.start()
    got = [net.copy(st, mine, net.mate(k)) for k in range(1, NR)]
    own.wait()
    for g in got:
        g.wait_recv()
    net.finish()


def scatter_steps(net, h, dq, w, dx, s1, r1, s2, r2, own, r3, r4):
    first, second = ('z', 'y') if h == 0 else ('y', 'z')
    f, g = (net.z, net.y) if h == 0 else (net.y, net.z)

    def part(ft, gt):
        c = ft * 4 + gt if h == 0 else gt * 4 + ft
        wb = w[c // 2, pl.ds(pl.multiple_of((c % 2) * HB, HB), HB), :]
        return dot(dq[pl.ds(h * HB, HB), :], wb, NT)

    def fill(dst, ft, base):
        def body(j, _):
            dst[j] = part(ft, base + j)
            return 0
        lax.fori_loop(0, dst.shape[0], body, 0)

    right, left = net.dev(first, 1), net.dev(first, 3)
    fill(s1.at[0], (f + 2) % 4, 0)
    fill(s1.at[1], (f + 2) % 4, 2)
    a = net.copy(s1.at[0], r1.at[0], right)
    b = net.copy(s1.at[1], r1.at[1], left)
    yield
    fill(s2.at[0], (f + 1) % 4, 0)
    a2 = net.copy(s2.at[0, pl.ds(2, 2)], r2.at[0, pl.ds(2, 2)], right)
    fill(s2.at[1], (f + 3) % 4, 0)
    b2 = net.copy(s2.at[1, pl.ds(0, 2)], r2.at[1, pl.ds(0, 2)], left)
    yield
    a.wait_recv()

    def add0(j, _):
        s2[0, j] = s2[0, j] + r1[0, j]
        return 0
    lax.fori_loop(0, 2, add0, 0)
    b.wait_recv()

    def add1(j, _):
        s2[1, 2 + j] = s2[1, 2 + j] + r1[1, j]
        return 0
    lax.fori_loop(0, 2, add1, 0)
    a = net.copy(s2.at[0, pl.ds(0, 2)], r2.at[0, pl.ds(0, 2)], right)
    b = net.copy(s2.at[1, pl.ds(2, 2)], r2.at[1, pl.ds(2, 2)], left)
    fill(own, f, 0)
    yield
    for cp in (a2, b2, a, b):
        cp.wait_recv()

    def add2(j, _):
        own[j] = own[j] + r2[0, j] + r2[1, j]
        return 0
    lax.fori_loop(0, 4, add2, 0)
    right, left = net.dev(second, 1), net.dev(second, 3)
    go, gr, gl = (g + 2) % 4, (g + 1) % 4, (g + 3) % 4
    up, low = pl.ds(0, LANE), pl.ds(LANE, LANE)
    a = net.copy(own.at[go, up], r3.at[0], right)
    b = net.copy(own.at[go, low], r3.at[1], left)
    a2 = net.copy(own.at[gr, low], r4.at[0, low], right)
    b2 = net.copy(own.at[gl, up], r4.at[1, up], left)
    yield
    a.wait_recv()
    own[gr, up, :] = own[gr, up, :] + r3[0]
    b.wait_recv()
    own[gl, low, :] = own[gl, low, :] + r3[1]
    a = net.copy(own.at[gr, up], r4.at[0, up], right)
    b = net.copy(own.at[gl, low], r4.at[1, low], left)
    yield
    for cp in (a2, b2, a, b):
        cp.wait_recv()
    dx[h] = (own[g] + r4[0] + r4[1]).astype(BF)


def back(dq, o, wg, xtg, dytg, dx, dw, dwt, *scr):
    bufs, (w, xt, dyt, og, dqg, acc, acco, dwo, send, recv, local) = scr[:14], scr[14:]
    loads = [pltpu.make_async_copy(a, b, local.at[i]) for i, (a, b) in enumerate(((wg, w), (dytg, dyt), (xtg, xt)))]
    for cp in loads:
        cp.start()
    net = Net(send, recv)
    net.tail = []
    net.enter(('x', 'z', 'y', 'core'), True)
    net.n = 2

    def go(*gens):
        for g in gens:
            next(g, None)

    gog = row_steps(net, o, og, half_rows(HB), None)
    gdq = row_steps(net, dq, dqg, half_rows(HB), None)
    rs0 = scatter_steps(net, 0, dq, w, dx, *bufs[:7])
    rs1 = scatter_steps(net, 1, dq, w, dx, *bufs[7:])
    gsw = swap_steps(net, dwo, dwt, 0)
    go(gog, gdq)
    loads[0].wait()
    go(rs0, rs1, rs0, rs1, gog, rs0, rs1, gog, gog)
    loads[1].wait()

    def tokens(ref, r, k):
        return ref[:, :, r // 4, r % 4, k].reshape(SB, HB)

    def dwo_step(r, a):
        for k in range(2):
            acco[k] += dot(og[r], tokens(dyt, r, k), TN)
        return a
    acco[...] = jnp.zeros_like(acco)
    lax.fori_loop(0, NR, dwo_step, 0)
    dwo[...] = acco[...].astype(BF)
    go(gdq, gsw, gdq, gdq)
    loads[2].wait()

    def dw_step(r, a):
        for k in range(2):
            acc[pl.ds(k * HB, HB), :] += dot(tokens(xt, r, k), dqg[r], TN)
        return a
    acc[...] = jnp.zeros_like(acc)
    go(rs0, rs1)
    lax.fori_loop(0, NR // 2, dw_step, 0)
    go(rs0, rs1)
    lax.fori_loop(NR // 2, NR, dw_step, 0)
    dw[...] = acc[...].astype(BF)
    go(rs0, rs1, gsw)
    for g in (gog, gdq, rs0, rs1, gsw):
        for _ in g:
            pass
    net.finish()
    for f in net.tail:
        f()


def doc_of(pos, c1, c2):
    return (pos >= c1).astype(jnp.int32) + (pos >= c2).astype(jnp.int32)


def bounds(r, c1, c2):
    p0, p1 = r * SB, r * SB + SB - 1
    lo = jnp.where(p0 >= c2, c2, jnp.where(p0 >= c1, c1, 0))
    hi = jnp.where(p1 >= c2, NR * SB, jnp.where(p1 >= c1, c2, c1))
    return lo // SB, (hi + SB - 1) // SB


def cuts_of(seg):
    return [jnp.sum((seg[...] < d).astype(F32)).astype(jnp.int32) // 2 for d in (1, 2)]


def tile(t):
    return slice(t * LANE, (t + 1) * LANE)


def attend(seg, ag, ado, o, dq, st, s_scr, d_scr, m_scr, l_scr, e_scr, o_scr, q_scr):
    r = lax.axis_index('row')
    c1, c2 = cuts_of(seg)
    lo, hi = bounds(r, c1, c2)
    qdoc = doc_of(r * SB + lax.broadcasted_iota(jnp.int32, (SB, LANE), 0), c1, c2)
    st[...] = jnp.zeros_like(st)
    for h in range(2):
        b = h * HQKV
        m_scr[...] = jnp.full(m_scr.shape, -jnp.inf, F32)
        l_scr[...] = jnp.zeros_like(l_scr)
        e_scr[...] = jnp.zeros_like(e_scr)
        o_scr[...] = jnp.zeros_like(o_scr)
        q_scr[...] = jnp.zeros_like(q_scr)

        def sweep1(kb, _):
            s = dot(ag[r, :, b:b + LANE], ag[kb, :, b + LANE:b + HB], NT) * SCALE
            m = m_scr[...]
            for t in range(4):
                kdoc = doc_of(kb * SB + t * LANE + lax.broadcasted_iota(jnp.int32, (1, LANE), 1), c1, c2)
                v = jnp.where(qdoc == kdoc, s[:, tile(t)], -jnp.inf)
                s_scr[kb, :, tile(t)] = v
                m = jnp.maximum(m, v)
            m_scr[...] = m
            return 0
        lax.fori_loop(lo, hi, sweep1, 0)
        m_scr[...] = jnp.broadcast_to(jnp.max(m_scr[...], axis=1, keepdims=True), m_scr.shape)

        def sweep2(kb, _):
            d = dot(ado[r, :, h * LANE:(h + 1) * LANE], ag[kb, :, b + HB:b + HQKV], NT)
            l, e, m = l_scr[...], e_scr[...], m_scr[...]
            for t in range(4):
                p = jnp.exp(s_scr[kb, :, tile(t)] - m)
                s_scr[kb, :, tile(t)] = p
                d_scr[kb, :, tile(t)] = d[:, tile(t)]
                l = l + p
                e = e + p * d[:, tile(t)]
            l_scr[...] = l
            e_scr[...] = e
            return 0
        lax.fori_loop(lo, hi, sweep2, 0)
        tot = jnp.sum(l_scr[...], axis=1, keepdims=True)
        dot_row = jnp.sum(e_scr[...], axis=1, keepdims=True) / tot
        lse = jnp.broadcast_to(m_scr[:, 0:1] + jnp.log(tot), m_scr.shape)
        st[h:h + 1, :] = jnp.transpose(lse)[0:1, :]
        l_scr[...] = jnp.broadcast_to(1.0 / tot, l_scr.shape)
        e_scr[...] = jnp.broadcast_to(dot_row, e_scr.shape)
        st[2 + h:3 + h, :] = jnp.transpose(e_scr[...])[0:1, :]

        def sweep3(kb, _):
            ps, ds = [], []
            for t in range(4):
                p = s_scr[kb, :, tile(t)] * l_scr[...]
                ps.append(p.astype(BF))
                ds.append((p * (d_scr[kb, :, tile(t)] - e_scr[...]) * SCALE).astype(BF))
            o_scr[...] += dot(jnp.concatenate(ps, axis=1), ag[kb, :, b + HB:b + HQKV])
            q_scr[...] += dot(jnp.concatenate(ds, axis=1), ag[kb, :, b + LANE:b + HB])
            return 0
        lax.fori_loop(lo, hi, sweep3, 0)
        o[:, h * LANE:(h + 1) * LANE] = o_scr[...].astype(BF)
        dq[:, h * LANE:(h + 1) * LANE] = q_scr[...].astype(BF)


def attend_t(seg, ag, ado, sg, dq, out, k_scr, v_scr):
    r = lax.axis_index('row')
    c1, c2 = cuts_of(seg)
    lo, hi = bounds(r, c1, c2)
    kdoc = doc_of(r * SB + lax.broadcasted_iota(jnp.int32, (SB, LANE), 0), c1, c2)
    for h in range(2):
        b = h * HQKV
        k_scr[...] = jnp.zeros_like(k_scr)
        v_scr[...] = jnp.zeros_like(v_scr)

        def sweep(qb, _):
            q, do = ag[qb, :, b:b + LANE], ado[qb, :, h * LANE:(h + 1) * LANE]
            s = dot(ag[r, :, b + LANE:b + HB], q, NT) * SCALE
            d = dot(ag[r, :, b + HB:b + HQKV], do, NT)
            ps, ds = [], []
            for t in range(4):
                qdoc = doc_of(qb * SB + t * LANE + lax.broadcasted_iota(jnp.int32, (1, LANE), 1), c1, c2)
                v = s[:, tile(t)] - sg[qb, h:h + 1, tile(t)]
                p = jnp.exp(jnp.where(kdoc == qdoc, v, -jnp.inf))
                ps.append(p.astype(BF))
                ds.append((p * (d[:, tile(t)] - sg[qb, 2 + h:3 + h, tile(t)]) * SCALE).astype(BF))
            v_scr[...] += dot(jnp.concatenate(ps, axis=1), do)
            k_scr[...] += dot(jnp.concatenate(ds, axis=1), q)
            return 0
        lax.fori_loop(lo, hi, sweep, 0)
        out[:, b:b + LANE] = dq[:, h * LANE:(h + 1) * LANE]
        out[:, b + LANE:b + HB] = k_scr[...].astype(BF)
        out[:, b + HB:b + HQKV] = v_scr[...].astype(BF)


def emit(*refs):
    for i in range(3):
        refs[3 + i][...] = refs[i][...]


def vm():
    return pl.BlockSpec(memory_space=pltpu.VMEM)


def hb():
    return pl.BlockSpec(memory_space=pl.ANY)


def sds(shape, dtype=BF):
    return jax.ShapeDtypeStruct(shape, dtype)


def net_call(fn, args, outs, cid, copies, n_local, scratch=(), out_specs=None, in_specs=None):
    return pl.pallas_call(
        fn, out_shape=outs, in_specs=in_specs or [vm()] * len(args),
        out_specs=out_specs or [hb()] * len(outs),
        scratch_shapes=[*scratch, pltpu.SemaphoreType.DMA((copies,)), pltpu.SemaphoreType.DMA((copies,)),
                        pltpu.SemaphoreType.DMA((n_local,))],
        compiler_params=pltpu.CompilerParams(collective_id=cid, has_side_effects=True, vmem_limit_bytes=VLIM),
    )(*args)


def core_call(fn, args, out, scratch):
    specs = [vm()] * len(args)
    return pl.pallas_call(
        fn, out_shape=out, in_specs=specs, out_specs=jax.tree.map(lambda _: vm(), out),
        scratch_shapes=scratch, compiler_params=pltpu.CompilerParams(vmem_limit_bytes=VLIM))(*args)


def grad_step(x_blk, wqkv_blk, wout_blk, seg_blk, dy_blk):
    x3, dy3, wo3 = (a.reshape(2, HB, HB) for a in (x_blk, dy_blk, wout_blk))
    seg8 = jnp.concatenate([seg_blk, seg_blk]).reshape(8, LANE)
    piece = (2, HB, HB)
    part = (2, 4, 2, TOK, HB)
    gathered = (NC, NR, 2, TOK, HB)
    plane = pltpu.VMEM((4, 4) + piece, BF)
    segg, wg, ag, ado, xtg, dytg = net_call(
        front, (x3, dy3, wqkv_blk, wo3, seg8),
        (sds((NR, 8, LANE), jnp.int32), sds((NR, SB, QKV)), sds((NR, SB, QKV)), sds((NR, SB, HB)),
         sds((4, 4) + part), sds((4, 4) + part)),
        cid=1, copies=162, n_local=8,
        scratch=[plane, plane, pltpu.VMEM((NR, SB, QKV), BF), pltpu.VMEM((NR,) + piece, BF), pltpu.VMEM(piece, BF),
                 pltpu.VMEM(part, BF), pltpu.VMEM(part, BF), pltpu.VMEM((SB, QKV), F32),
                 pltpu.VMEM((SB, QKV), BF), pltpu.VMEM((SB, HB), BF)])
    row128 = pltpu.VMEM((SB, LANE), F32)
    o, dq, st = core_call(
        attend, (segg, ag, ado), (sds((SB, HB)), sds((SB, HB)), sds((8, SB), F32)),
        [pltpu.VMEM((NR, SB, SB), F32), pltpu.VMEM((NR, SB, SB), F32)] + [row128] * 5)
    sg, = net_call(share, (st,), (sds((NR, 8, SB), F32),), cid=3, copies=7, n_local=1)
    dqkv = core_call(attend_t, (segg, ag, ado, sg, dq), sds((SB, QKV)), [row128] * 2)
    b2, b4 = pltpu.VMEM((2,) + piece, F32), pltpu.VMEM((2, 4, HB, HB), F32)
    bufs = [b2, b2, b4, b4, pltpu.VMEM((4, HB, HB), F32), pltpu.VMEM((2, LANE, HB), F32), pltpu.VMEM(piece, F32)]
    tokens = pltpu.VMEM((4, 4) + part, BF)
    dx, dw, dwt = net_call(
        back, (dqkv, o, wg, xtg, dytg), (sds(piece), sds((SB, QKV)), sds(piece)), cid=4, copies=46, n_local=3,
        scratch=bufs * 2 + [pltpu.VMEM((NR, SB, QKV), BF), tokens, tokens, pltpu.VMEM((NR, SB, HB), BF),
                            pltpu.VMEM((NR, SB, QKV), BF), pltpu.VMEM((SB, QKV), F32), pltpu.VMEM(piece, F32),
                            pltpu.VMEM(piece, BF)],
        in_specs=[vm()] * 2 + [hb()] * 3, out_specs=[vm()] * 3)
    small = sds((SB, HB))
    return core_call(emit, (dx.reshape(SB, HB), dw, dwt.reshape(SB, HB)), (small, sds((SB, QKV)), small), [])


def solution(mesh):
    tok_spec = P(('dp', 'row'), 'col')
    mat_spec = P('row', 'col')
    seg_spec = P(('dp', 'row'))
    return jax.shard_map(grad_step, mesh=mesh, in_specs=(tok_spec, mat_spec, mat_spec, seg_spec, tok_spec),
                         out_specs=(tok_spec, tok_spec, tok_spec), check_vma=False)
```
